32 devices in a mesh: tm: 16 (over z, y, x), head: 2 (over core).
Axes of the slice: x: 2, y: 2, z: 4, core: 2. Of those that a mesh axis runs over, the one named last changes fastest.
Arguments:
- queries: bfloat16 [2048, 6144], P('tm', 'head'), may hold values from -150 to 150
- window_keys: bfloat16 [2048, 6144], P('tm', 'head'), may hold values from -6 to 6
- window_values: bfloat16 [2048, 6144], P('tm', 'head'), may hold values from -6 to 6
- context_keys: bfloat16 [2048, 6144], P('tm', 'head'), may hold values from -6 to 6
- context_values: bfloat16 [2048, 6144], P('tm', 'head'), may hold values from -6 to 6
- block_group: int32 [64], replicated, may hold values from 0 to 15, never falling along the last dimension, each value on 1 to 8 neighbouring positions
- sees: int32 [16, 16], replicated, may hold values from 0 to 1, as said below
- out_weight: bfloat16 [6144, 6144], P('head'), may hold values from -1 to 1
- gate: float32 [6144], P('head'), may hold values from 0.5 to 2
Outputs:
- update: bfloat16 [2048, 6144], P('tm', 'head')
The draws below stay inside these ranges and needn't reach their ends.
Inputs may be any that keep to these rules, and one draw needn't show every extreme that they name: sees[a, a] is 1 and sees[a, b] is 0 for b > a. `block_group`: never falling along the blocks.
All inputs are finite; a program needn't handle non-finite values.
Results may differ from the reference program's by a relative error of at most 0.03.
Values may be sent and summed in bfloat16 or wider, within the bound.
No kernel may reach another device: no remote copies, remote signals or barrier semaphores. Data moves between devices by JAX's collectives and lax.ppermute only.
A program may use at most 192 MiB of HBM per device.

```python
import math
import jax
import jax.numpy as jnp
import numpy as np
from jax import lax

HEADS = 48
HD = 128
D = 6144
BLOCK = 64
WIN = 2048
CTX = 2048
NBLK = 64
NCHUNK = 16


def pair_draw(key):
    query_key = jax.random.fold_in(key, 11)
    window_key = jax.random.fold_in(key, 12)
    keys_drawn = jnp.clip(jax.random.normal(window_key, (WIN, D), jnp.float32), -6.0, 6.0)
    queries_drawn = jnp.clip(jax.random.normal(query_key, (WIN, D), jnp.float32), -6.0, 6.0)
    return (queries_drawn, keys_drawn)


def draw_queries(key, part):
    return pair_draw(key)[0].astype(jnp.bfloat16)


def draw_window_keys(key, part):
    return pair_draw(key)[1].astype(jnp.bfloat16)


def draw_sees(key, part):
    coins = jax.random.randint(jax.random.fold_in(key, 21), (NCHUNK, NCHUNK), 0, 4)
    row_ids = jnp.arange(NCHUNK, dtype=jnp.int32)[:, None]
    col_ids = jnp.arange(NCHUNK, dtype=jnp.int32)[None, :]
    lower = jnp.where(coins != 0, 1, 0).astype(jnp.int32)
    return jnp.where(row_ids == col_ids, 1, jnp.where(row_ids > col_ids, lower, 0)).astype(jnp.int32)


def shard_levels(own_key, dims, pieces, low, high):
    def one(dim, parts):
        heights = jax.random.uniform(jax.random.fold_in(jax.random.fold_in(own_key, 6), dim), (parts,), jnp.float32, low / len(pieces), high / len(pieces))
        return jnp.repeat(jnp.exp(heights), dims[dim] // parts).reshape((-1,) + (1,) * (len(dims) - dim - 1))

    level = one(*pieces[0])
    for cut in pieces[1:]:
        level = level * one(*cut)
    return level


def split_up(amount, total, reach, slope):
    weights = [(1 << 20) // math.isqrt(grade ** slope) + 1 for grade in range(2, amount + 1)]
    spare, given = total - reach - (amount - 1), [1] * (amount - 1)
    while spare > 0:
        movable = [i for i in range(amount - 1) if given[i] < reach]
        pool, left = sum([weights[i] for i in movable]), spare
        for i in movable:
            more = min(reach - given[i], max(1, left * weights[i] // pool), spare)
            given[i] = given[i] + more
            spare = spare - more
    return np.array([reach] + given)


def uneven_parts(stream_key, amount, total, most, lean):
    if amount == 2:
        one = jax.random.randint(stream_key, (), max(1, total - most), min(most, total - 1) + 1)
        return jnp.stack([one, total - one])
    sizes = jnp.asarray(split_up(amount, total, most, lean), jnp.int32)
    couples = (amount - 1) // 2
    donor, taker = sizes[1:1 + 2 * couples:2], sizes[2:2 + 2 * couples:2]
    room = jnp.minimum(donor - 1, most - taker)
    passed = jax.random.randint(jax.random.fold_in(stream_key, 1), (couples,), 0, 1 << 20) % (room + 1)
    sizes = sizes.at[1:1 + 2 * couples:2].set(donor - passed).at[2:2 + 2 * couples:2].set(taker + passed)
    return sizes[jax.random.permutation(jax.random.fold_in(stream_key, 2), amount)]


def centred(own_key, shape, width, most, cuts=(), held_as=jnp.bfloat16):
    drawn = jax.random.normal(own_key, shape, jnp.float32) * width
    if len(cuts) > 0:
        drawn = shard_levels(own_key, shape, cuts, -0.22, 0.18) * drawn
    return jnp.clip(drawn, min=-most, max=most).astype(held_as)


def setup_inputs(seed: int = 0) -> dict:
    arg_keys = jax.random.split(jax.random.key(seed), 10)
    return {
        "queries": draw_queries(jax.random.fold_in(arg_keys[9], 71), 0),
        "window_keys": draw_window_keys(jax.random.fold_in(arg_keys[9], 71), 0),
        "window_values": centred(arg_keys[2], (WIN, D), 1.0, 6.0, ((0, 16), (1, 2))),
        "context_keys": centred(arg_keys[3], (CTX, D), 1.0, 6.0, ((0, 16), (1, 2))),
        "context_values": centred(arg_keys[4], (CTX, D), 1.0, 6.0, ((0, 16), (1, 2))),
        "block_group": jnp.searchsorted(jnp.cumsum(uneven_parts(arg_keys[5], NCHUNK, NBLK, 8, 1)), jnp.arange(NBLK), side="right").astype(jnp.int32),
        "sees": draw_sees(jax.random.fold_in(arg_keys[9], 71), 0),
        "out_weight": centred(arg_keys[7], (D, D), (HD // 4) ** -0.5, 1.0, ((0, 2),)),
        "gate": jnp.clip(0.5 + 1.5 * jax.random.uniform(arg_keys[8], (D,), jnp.float32) ** shard_levels(arg_keys[8], (D,), ((0, 2),), -0.2, 0.2), 0.5, 2.0),
    }


def group_mask(block_group, sees):
    positions = jnp.arange(CTX + WIN, dtype=jnp.int32)
    key_groups = block_group[positions // BLOCK]
    query_groups = key_groups[CTX:]
    return sees[query_groups][:, key_groups] > 0

def reference(queries, window_keys, window_values, context_keys, context_values, block_group, sees, out_weight, gate):
    all_keys = jnp.concatenate([context_keys, window_keys], axis=0)
    all_values = jnp.concatenate([context_values, window_values], axis=0)
    visible = group_mask(block_group, sees)
    score_scale = 1.0 / jnp.sqrt(jnp.float32(HD))

    def one_head(head_id):
        start = (head_id * HD).astype(jnp.int32)
        query_h = lax.dynamic_slice_in_dim(queries, start, HD, 1)
        key_h = lax.dynamic_slice_in_dim(all_keys, start, HD, 1)
        value_h = lax.dynamic_slice_in_dim(all_values, start, HD, 1)
        scores = jnp.dot(query_h, key_h.T, preferred_element_type=jnp.float32) * score_scale
        scores = jnp.where(visible, scores, jnp.float32(-1e+30))
        row_peak = lax.optimization_barrier(jnp.max(scores, axis=-1, keepdims=True))
        weights = jnp.where(visible, jnp.exp(scores - row_peak), jnp.float32(0.0))
        row_total = lax.optimization_barrier(jnp.sum(weights, axis=-1, keepdims=True))
        numer = jnp.dot(weights.astype(jnp.bfloat16), value_h, preferred_element_type=jnp.float32)
        return (numer / row_total).astype(jnp.bfloat16)
    per_head = lax.map(one_head, jnp.arange(HEADS, dtype=jnp.int32))
    attended = jnp.transpose(per_head, (1, 0, 2)).reshape(WIN, D)
    projected = jnp.dot(attended, out_weight, preferred_element_type=jnp.float32)
    return (gate[None, :] * projected).astype(jnp.bfloat16)
```

```python
import functools
import math

import jax
import jax.numpy as jnp
from jax import lax
from jax.experimental import pallas as pl
from jax.experimental.pallas import tpu as pltpu
from jax.sharding import PartitionSpec as P

HD = 128
BLOCK = 64
MASKED = -1e30
VMEM_LIMIT = 48 * 1024 * 1024


def group_rows(positions, group_table, group_count):
    blocks = positions // BLOCK
    picker = (blocks[:, None] == jnp.arange(group_table.shape[0], dtype=jnp.int32)[None, :]).astype(
        jnp.float32
    )
    group_ids = jnp.dot(picker, group_table, precision=lax.Precision.HIGHEST)
    return (group_ids[:, None] == jnp.arange(group_count, dtype=jnp.float32)[None, :]).astype(
        jnp.float32
    )


def gathered_body(
    queries,
    window_keys,
    window_values,
    context_keys,
    context_values,
    block_group,
    sees,
    out_weight,
    gate,
):
    tok_rows = queries.shape[0]
    features = queries.shape[1]
    local_heads = features // HD
    tm_count = lax.axis_size("tm")
    own_index = lax.axis_index("tm")
    ctx_rows = context_keys.shape[0]
    ctx_total = ctx_rows * tm_count
    group_count = sees.shape[0]
    group_table = block_group.astype(jnp.float32)
    sees_table = sees.astype(jnp.float32)
    score_scale = 1.0 / jnp.sqrt(jnp.float32(HD))
    all_queries = lax.all_gather(queries, "tm", axis=0, tiled=True)
    win_rows = all_queries.shape[0]
    query_pos = ctx_total + jnp.arange(win_rows, dtype=jnp.int32)
    key_pos = jnp.concatenate(
        [
            own_index * ctx_rows + jnp.arange(ctx_rows, dtype=jnp.int32),
            ctx_total + own_index * tok_rows + jnp.arange(tok_rows, dtype=jnp.int32),
        ]
    )
    query_sees = jnp.dot(
        group_rows(query_pos, group_table, group_count), sees_table, precision=lax.Precision.HIGHEST
    )
    key_onehot = group_rows(key_pos, group_table, group_count)
    visible = jnp.dot(query_sees, key_onehot.T, precision=lax.Precision.HIGHEST) > 0.5
    key_piece = jnp.concatenate([context_keys, window_keys], axis=0).reshape(
        ctx_rows + tok_rows, local_heads, HD
    )
    value_piece = jnp.concatenate([context_values, window_values], axis=0).reshape(
        ctx_rows + tok_rows, local_heads, HD
    )
    query_heads = all_queries.reshape(win_rows, local_heads, HD)
    scores = (
        jnp.einsum("qhd,khd->hqk", query_heads, key_piece, preferred_element_type=jnp.float32)
        * score_scale
    )
    scores = jnp.where(visible[None], scores, jnp.float32(-1e30))
    row_peak = lax.pmax(jnp.max(scores, axis=-1).astype(jnp.bfloat16), "tm").astype(jnp.float32)
    weights = jnp.where(visible[None], jnp.exp(scores - row_peak[..., None]), jnp.float32(0.0))
    totals = jnp.sum(weights, axis=-1).T
    numer = jnp.einsum(
        "hqk,khd->qhd",
        weights.astype(jnp.bfloat16),
        value_piece,
        preferred_element_type=jnp.float32,
    ).reshape(win_rows, features)
    numer_mine, totals_mine = (
        lax.psum_scatter(numer.astype(jnp.bfloat16), "tm", scatter_dimension=0, tiled=True).astype(
            jnp.float32
        ),
        lax.psum_scatter(totals.astype(jnp.bfloat16), "tm", scatter_dimension=0, tiled=True).astype(
            jnp.float32
        ),
    )
    attended = (
        (numer_mine.reshape(tok_rows, local_heads, HD) / totals_mine[..., None])
        .reshape(tok_rows, features)
        .astype(jnp.bfloat16)
    )
    projected = jnp.dot(attended, out_weight, preferred_element_type=jnp.float32)
    summed = lax.psum_scatter(
        projected.astype(jnp.bfloat16), "head", scatter_dimension=1, tiled=True
    ).astype(jnp.float32)
    return (gate[None, :] * summed).astype(jnp.bfloat16)


def pack_kernel(q_ref, ck_ref, wk_ref, cv_ref, wv_ref, shared_ref, own_ref):
    at_shared, at_own = 0, 0
    for ref in (q_ref, ck_ref, wk_ref, cv_ref, wv_ref):
        rows = ref.shape[0]
        half = rows // 2
        for side in range(2):
            shared_ref[side, at_shared : at_shared + half, :] = ref[
                side * half : (side + 1) * half, HD : 2 * HD
            ]
            own_ref[side, at_own : at_own + rows, :] = ref[:, 2 * side * HD : (2 * side + 1) * HD]
        at_shared += half
        at_own += rows


def pack(q, ck, wk, cv, wv):
    pairs = q.shape[1] // (3 * HD)
    rows = [x.shape[0] for x in (q, ck, wk, cv, wv)]
    total = sum(rows)
    return pl.pallas_call(
        pack_kernel,
        grid=(pairs,),
        in_specs=[pl.BlockSpec((r, 3 * HD), lambda j: (0, j)) for r in rows],
        out_specs=[
            pl.BlockSpec((2, total // 2, HD), lambda j: (j, 0, 0)),
            pl.BlockSpec((2, total, HD), lambda j: (j, 0, 0)),
        ],
        out_shape=[
            jax.ShapeDtypeStruct((2 * pairs, total // 2, HD), q.dtype),
            jax.ShapeDtypeStruct((2 * pairs, total, HD), q.dtype),
        ],
        name="pack",
    )(q, ck, wk, cv, wv)


def attend_kernel(q_from, q_rows, sources, scale, *refs):
    n = len(sources)
    operands, bias_ref, out_ref, k_all, v_all = (
        refs[:n],
        refs[n],
        refs[n + 1],
        refs[n + 2],
        refs[n + 3],
    )
    step = pl.program_id(0)

    @pl.when(step == 0)
    def _():
        at = 0
        for ref, (k_lo, k_hi, v_lo, v_hi) in zip(operands, sources):
            count = ref.shape[0] * (k_hi - k_lo)
            k_all[at : at + count, :] = ref[:, k_lo:k_hi, :].reshape(count, HD)
            v_all[at : at + count, :] = ref[:, v_lo:v_hi, :].reshape(count, HD)
            at += count

    chips = out_ref.shape[0]
    tile = chips * q_rows
    runs = bias_ref.shape[1]
    keys = k_all.shape[0]
    q = operands[0][pl.ds(step * chips, chips), q_from : q_from + q_rows, :].reshape(tile, HD)
    scores = lax.dot_general(
        q, k_all[...], (((1,), (1,)), ((), ())), preferred_element_type=jnp.float32
    )
    scores = scores.reshape(runs, tile // runs, keys) * scale + bias_ref[0][:, None, :]
    peak = jnp.max(scores, axis=-1, keepdims=True)
    weights = jnp.exp2(scores - peak)
    total = jnp.sum(weights, axis=-1, keepdims=True).reshape(tile, 1)
    numer = jnp.dot(
        weights.astype(jnp.bfloat16).reshape(tile, keys),
        v_all[...],
        preferred_element_type=jnp.float32,
    )
    out_ref[...] = (numer / total).astype(out_ref.dtype).reshape(out_ref.shape)


def attend(operands, sources, bias, q_from, q_rows, tile_rows, name):
    count = operands[0].shape[0]
    chips = tile_rows // q_rows
    keys = bias.shape[1]
    runs = tile_rows // BLOCK
    bias = bias.reshape(bias.shape[0] // runs, runs, keys)
    scale = math.log2(math.e) / math.sqrt(HD)
    work = count * q_rows * keys
    return pl.pallas_call(
        functools.partial(attend_kernel, q_from, q_rows, sources, scale),
        grid=(count // chips,),
        in_specs=[pl.BlockSpec(x.shape, lambda i: (0, 0, 0)) for x in operands]
        + [pl.BlockSpec((1, runs, keys), lambda i: (i, 0, 0))],
        out_specs=pl.BlockSpec((chips, q_rows, HD), lambda i: (i, 0, 0)),
        out_shape=jax.ShapeDtypeStruct((count, q_rows, HD), jnp.bfloat16),
        scratch_shapes=[pltpu.VMEM((keys, HD), jnp.bfloat16), pltpu.VMEM((keys, HD), jnp.bfloat16)],
        cost_estimate=pl.CostEstimate(
            flops=8 * work * HD, bytes_accessed=4 * 1024 * 1024, transcendentals=work
        ),
        compiler_params=pltpu.CompilerParams(vmem_limit_bytes=VMEM_LIMIT),
        name=name,
    )(*operands, bias)


def project_kernel(which_ref, shared_ref, own_lo_ref, own_hi_ref, w_ref, out_ref, acc_ref):
    step = pl.program_id(0)
    rows = shared_ref.shape[0] * shared_ref.shape[1]

    @pl.when(step == 0)
    def _():
        acc_ref[...] = jnp.zeros_like(acc_ref)

    left = jnp.concatenate([own_lo_ref[0], own_hi_ref[0]], axis=0)
    middle = shared_ref[...].reshape(rows, HD)
    right = jnp.concatenate([own_lo_ref[1], own_hi_ref[1]], axis=0)
    attended = jnp.concatenate([left, middle, right], axis=1)
    acc_ref[...] += jnp.dot(attended, w_ref[...], preferred_element_type=jnp.float32)

    @pl.when(step == pl.num_programs(0) - 1)
    def _():
        out_ref[...] = acc_ref[...].astype(out_ref.dtype)


def project(shared, own_lo, own_hi, weight, which, columns, dtype, name):
    pairs = shared.shape[0] // 2
    half = shared.shape[1]
    part = pl.BlockSpec((2, half, HD), lambda j, which: (j, 0, 0))
    return pl.pallas_call(
        project_kernel,
        grid_spec=pltpu.PrefetchScalarGridSpec(
            num_scalar_prefetch=1,
            grid=(pairs,),
            in_specs=[
                part,
                part,
                part,
                pl.BlockSpec((3 * HD, columns), lambda j, which: (j, which[0])),
            ],
            out_specs=pl.BlockSpec((2 * half, columns), lambda j, which: (0, 0)),
            scratch_shapes=[pltpu.VMEM((2 * half, columns), jnp.float32)],
        ),
        out_shape=jax.ShapeDtypeStruct((2 * half, columns), dtype),
        cost_estimate=pl.CostEstimate(
            flops=4 * half * weight.shape[0] * columns,
            bytes_accessed=2 * weight.shape[0] * columns,
            transcendentals=0,
        ),
        compiler_params=pltpu.CompilerParams(vmem_limit_bytes=VMEM_LIMIT),
        name=name,
    )(which, shared, own_lo, own_hi, weight)


def dealt_body(
    queries,
    window_keys,
    window_values,
    context_keys,
    context_values,
    block_group,
    sees,
    out_weight,
    gate,
):
    tok_rows = queries.shape[0]
    ctx_rows = context_keys.shape[0]
    tm_count = lax.axis_size("tm")
    own_index = lax.axis_index("tm")
    core = lax.axis_index("head")
    side = own_index % 2
    half_q, half_c = tok_rows // 2, ctx_rows // 2

    shared, own = pack(queries, context_keys, window_keys, context_values, window_values)
    shared = lax.all_to_all(shared, "tm", 0, 0, tiled=True)
    own = lax.all_to_all(own, "tm", 0, 0, tiled=True)

    table = sees.astype(jnp.float32)
    groups = jnp.arange(sees.shape[0], dtype=jnp.int32)
    picks = (block_group[:, None] == groups[None, :]).astype(jnp.float32)
    ctx_blocks = ctx_rows * tm_count // BLOCK
    can_see = picks[ctx_blocks:] @ table @ picks.T
    bias_blocks = jnp.where(can_see > 0.5, jnp.float32(0.0), jnp.float32(MASKED))
    n_query_blocks = bias_blocks.shape[0]

    def by_device(x, rows):
        return x.reshape(n_query_blocks, tm_count, rows // BLOCK)

    ctx_part = by_device(bias_blocks[:, :ctx_blocks], ctx_rows)
    win_part = by_device(bias_blocks[:, ctx_blocks:], tok_rows)
    spread = lambda x: jnp.broadcast_to(
        x.reshape(x.shape[0], -1)[:, :, None], (x.shape[0], x[0].size, BLOCK)
    ).reshape(x.shape[0], -1)
    own_bias = spread(jnp.concatenate([ctx_part, win_part], axis=2))
    own_bias = own_bias.reshape(tm_count, 2, half_q // BLOCK, -1)
    own_bias_lo = own_bias[:, 0].reshape(n_query_blocks // 2, -1)
    own_bias_hi = own_bias[:, 1].reshape(n_query_blocks // 2, -1)

    def one_half(x, rows, which):
        blocks = rows // 2 // BLOCK
        return lax.dynamic_slice_in_dim(x, which * blocks, blocks, 2)

    shared_rows = []
    for which in (side, 1 - side):
        shared_rows.append(
            jnp.concatenate(
                [one_half(ctx_part, ctx_rows, which), one_half(win_part, tok_rows, which)], axis=2
            ).reshape(n_query_blocks, -1)
        )
    shared_blocks = jnp.concatenate(shared_rows, axis=1).reshape(
        tm_count, tok_rows // BLOCK, -1
    )
    shared_blocks = lax.dynamic_slice_in_dim(
        shared_blocks, side * (half_q // BLOCK), half_q // BLOCK, 1
    ).reshape(n_query_blocks // 2, -1)
    shared_bias = spread(shared_blocks)

    theirs = lax.ppermute(shared[:, half_q:, :], "tm", [(i, i ^ 1) for i in range(tm_count)])

    half_kv, full_kv = half_c + half_q, ctx_rows + tok_rows
    shared_out = attend(
        (shared, theirs),
        (
            (half_q, half_q + half_kv, half_q + half_kv, half_q + 2 * half_kv),
            (0, half_kv, half_kv, 2 * half_kv),
        ),
        shared_bias,
        0,
        half_q,
        4 * BLOCK,
        "attend_shared",
    )
    shared_out = lax.all_to_all(shared_out, "tm", 0, 0, tiled=True)
    own_source = ((tok_rows, tok_rows + full_kv, tok_rows + full_kv, tok_rows + 2 * full_kv),)
    own_lo = attend((own,), own_source, own_bias_lo, 0, half_q, 4 * BLOCK, "attend_lo")
    own_lo = lax.all_to_all(own_lo, "tm", 0, 0, tiled=True)
    own_hi = attend((own,), own_source, own_bias_hi, half_q, half_q, 4 * BLOCK, "attend_hi")
    own_hi = lax.all_to_all(own_hi, "tm", 0, 0, tiled=True)

    columns = gate.shape[0]
    other = (1 - core).astype(jnp.int32).reshape(1)
    mine = core.astype(jnp.int32).reshape(1)
    sent = project(
        shared_out, own_lo, own_hi, out_weight, other, columns, jnp.bfloat16, "project_theirs"
    )
    got = lax.ppermute(sent, "head", [(0, 1), (1, 0)])
    kept = project(
        shared_out, own_lo, own_hi, out_weight, mine, columns, jnp.float32, "project_mine"
    )
    return (gate[None, :] * (kept + got.astype(jnp.float32))).astype(jnp.bfloat16)


def body(queries, window_keys, window_values, context_keys, *rest):
    tm_count = lax.axis_size("tm")
    local_heads = queries.shape[1] // HD
    halves = (queries.shape[0] // 2, context_keys.shape[0] // 2)
    dealt = (
        2 * local_heads == 3 * tm_count
        and lax.axis_size("head") == 2
        and all(h % BLOCK == 0 for h in halves)
        and halves[0] * tm_count % (4 * BLOCK) == 0
    )
    chosen = dealt_body if dealt else gathered_body
    return chosen(queries, window_keys, window_values, context_keys, *rest)


def solution(mesh):
    placed = (
        P("tm", "head"),
        P("tm", "head"),
        P("tm", "head"),
        P("tm", "head"),
        P("tm", "head"),
        P(),
        P(),
        P("head", None),
        P("head"),
    )
    return jax.shard_map(
        body, mesh=mesh, in_specs=placed, out_specs=P("tm", "head"), check_vma=False
    )
```

```python
import functools
import math

import jax
import jax.numpy as jnp
from jax import lax
from jax.experimental import pallas as pl
from jax.experimental.pallas import tpu as pltpu
from jax.sharding import PartitionSpec as P

HD = 128
BLOCK = 64
MASKED = -1e30
VMEM_LIMIT = 40 * 1024 * 1024
TILE_ROWS = 4 * BLOCK
KEY_CHUNK = 256
ACCUMULATORS = 2
PROJECT_COLUMNS = 1024
PROJECT_PIECES = 6


def group_rows(positions, group_table, group_count):
    blocks = positions // BLOCK
    picker = (blocks[:, None] == jnp.arange(group_table.shape[0], dtype=jnp.int32)[None, :]).astype(
        jnp.float32
    )
    group_ids = jnp.dot(picker, group_table, precision=lax.Precision.HIGHEST)
    return (group_ids[:, None] == jnp.arange(group_count, dtype=jnp.float32)[None, :]).astype(
        jnp.float32
    )


def gathered_body(
    queries,
    window_keys,
    window_values,
    context_keys,
    context_values,
    block_group,
    sees,
    out_weight,
    gate,
):
    tok_rows = queries.shape[0]
    features = queries.shape[1]
    local_heads = features // HD
    tm_count = lax.axis_size("tm")
    own_index = lax.axis_index("tm")
    ctx_rows = context_keys.shape[0]
    ctx_total = ctx_rows * tm_count
    group_count = sees.shape[0]
    group_table = block_group.astype(jnp.float32)
    sees_table = sees.astype(jnp.float32)
    score_scale = 1.0 / jnp.sqrt(jnp.float32(HD))
    all_queries = lax.all_gather(queries, "tm", axis=0, tiled=True)
    win_rows = all_queries.shape[0]
    query_pos = ctx_total + jnp.arange(win_rows, dtype=jnp.int32)
    key_pos = jnp.concatenate(
        [
            own_index * ctx_rows + jnp.arange(ctx_rows, dtype=jnp.int32),
            ctx_total + own_index * tok_rows + jnp.arange(tok_rows, dtype=jnp.int32),
        ]
    )
    query_sees = jnp.dot(
        group_rows(query_pos, group_table, group_count), sees_table, precision=lax.Precision.HIGHEST
    )
    key_onehot = group_rows(key_pos, group_table, group_count)
    visible = jnp.dot(query_sees, key_onehot.T, precision=lax.Precision.HIGHEST) > 0.5
    key_piece = jnp.concatenate([context_keys, window_keys], axis=0).reshape(
        ctx_rows + tok_rows, local_heads, HD
    )
    value_piece = jnp.concatenate([context_values, window_values], axis=0).reshape(
        ctx_rows + tok_rows, local_heads, HD
    )
    query_heads = all_queries.reshape(win_rows, local_heads, HD)
    scores = (
        jnp.einsum("qhd,khd->hqk", query_heads, key_piece, preferred_element_type=jnp.float32)
        * score_scale
    )
    scores = jnp.where(visible[None], scores, jnp.float32(-1e30))
    row_peak = lax.pmax(jnp.max(scores, axis=-1).astype(jnp.bfloat16), "tm").astype(jnp.float32)
    weights = jnp.where(visible[None], jnp.exp(scores - row_peak[..., None]), jnp.float32(0.0))
    totals = jnp.sum(weights, axis=-1).T
    numer = jnp.einsum(
        "hqk,khd->qhd",
        weights.astype(jnp.bfloat16),
        value_piece,
        preferred_element_type=jnp.float32,
    ).reshape(win_rows, features)
    numer_mine, totals_mine = (
        lax.psum_scatter(numer.astype(jnp.bfloat16), "tm", scatter_dimension=0, tiled=True).astype(
            jnp.float32
        ),
        lax.psum_scatter(totals.astype(jnp.bfloat16), "tm", scatter_dimension=0, tiled=True).astype(
            jnp.float32
        ),
    )
    attended = (
        (numer_mine.reshape(tok_rows, local_heads, HD) / totals_mine[..., None])
        .reshape(tok_rows, features)
        .astype(jnp.bfloat16)
    )
    projected = jnp.dot(attended, out_weight, preferred_element_type=jnp.float32)
    summed = lax.psum_scatter(
        projected.astype(jnp.bfloat16), "head", scatter_dimension=1, tiled=True
    ).astype(jnp.float32)
    return (gate[None, :] * summed).astype(jnp.bfloat16)


def pack_kernel(whole, *refs):
    n = (len(refs) - 2) // 2
    in_refs, out_ref, held, sems = refs[:n], refs[n], refs[n + 1 : -1], refs[-1]
    copies = [pltpu.make_async_copy(x, y, sems.at[i]) for i, (x, y) in enumerate(zip(in_refs, held))]
    for copy in copies:
        copy.start()
    at = 0
    for copy, ref in zip(copies, held):
        copy.wait()
        rows = ref.shape[0]
        half = rows // 2
        for j in range(ref.shape[1] // (3 * HD)):
            for side in range(2):
                if whole:
                    head = 3 * j + 2 * side
                    out_ref[2 * j + side, at : at + rows, :] = ref[:, head * HD : (head + 1) * HD]
                else:
                    head = 3 * j + 1
                    out_ref[2 * j + side, at : at + half, :] = ref[
                        side * half : (side + 1) * half, head * HD : (head + 1) * HD
                    ]
        at += rows if whole else half


def pack(arrays, whole, name):
    groups = arrays[0].shape[1] // (3 * HD)
    rows = [x.shape[0] for x in arrays]
    total = sum(rows) if whole else sum(rows) // 2
    return pl.pallas_call(
        functools.partial(pack_kernel, whole),
        in_specs=[pl.BlockSpec(memory_space=pl.ANY) for _ in arrays],
        out_specs=pl.BlockSpec(memory_space=pltpu.VMEM),
        out_shape=jax.ShapeDtypeStruct((2 * groups, total, HD), arrays[0].dtype),
        scratch_shapes=[pltpu.VMEM(x.shape, x.dtype) for x in arrays]
        + [pltpu.SemaphoreType.DMA((len(arrays),))],
        cost_estimate=pl.CostEstimate(
            flops=1 << 29, bytes_accessed=8 * 1024 * 1024, transcendentals=0
        ),
        compiler_params=pltpu.CompilerParams(vmem_limit_bytes=VMEM_LIMIT),
        name=name,
    )(*arrays)


def attend_kernel(q_rows, keys_at, scale, carried, *refs):
    if carried:
        q_ref, kv_ref, bias_ref, mine_ref, theirs_ref, out_ref, k_all, v_all, kept_a, kept_b = refs
    else:
        q_ref, kv_ref, bias_ref, out_ref, k_all, v_all, kept_a, kept_b = refs
    keys = k_all.shape[0]
    chips = TILE_ROWS // q_rows
    runs = TILE_ROWS // BLOCK
    tiles = q_ref.shape[0] // chips
    half = q_rows // 2

    k_lo, k_hi, v_lo, v_hi = keys_at
    count = kv_ref.shape[0]
    k_all[:, :HD] = kv_ref[:, k_lo:k_hi, :].reshape(keys, HD)
    blocks = keys // BLOCK
    k_all[:, HD:] = (
        jnp.broadcast_to(bias_ref[...][:, None, :], (blocks, BLOCK, HD))
        .reshape(keys, HD)
        .astype(jnp.bfloat16)
    )
    some = v_hi - v_lo
    for i in range(count):
        v_all[:, i * some : (i + 1) * some] = kv_ref[i, v_lo:v_hi, :].T

    def finish(pair, odd, peak, total, numer):
        total = jnp.sum(total, axis=0, keepdims=True)
        numer = numer / total
        tile = 2 * pair + odd
        if not carried:
            out_ref[tile, :HD, :] = numer
            out_ref[tile, HD:, :] = jnp.broadcast_to(peak + jnp.log2(total), (8, TILE_ROWS))
            return
        side = TILE_ROWS // 2
        mine = mine_ref[pair, :, odd * side : (odd + 1) * side]
        theirs = theirs_ref[pair, :, odd * side : (odd + 1) * side]
        mine_log, their_log = mine[HD : HD + 1, :], theirs[HD : HD + 1, :]
        top = jnp.maximum(mine_log, their_log)
        mine_part, their_part = jnp.exp2(mine_log - top), jnp.exp2(their_log - top)
        joined = (mine_part * mine[:HD, :] + their_part * theirs[:HD, :]) / (mine_part + their_part)
        here = pl.ds(tile * chips, chips)
        out_ref[here, :half, :] = joined.T.astype(out_ref.dtype).reshape(chips, half, HD)
        out_ref[here, half:, :] = numer.T.astype(out_ref.dtype).reshape(chips, q_rows, HD)

    def advance(ahead, ahead_kept, pair, odd, peak, kept):
        if ahead is not None:
            q = q_ref[pl.ds(ahead * chips, chips), :q_rows, :].reshape(TILE_ROWS, HD).T
            row = lax.broadcasted_iota(jnp.int32, (HD, TILE_ROWS), 0)
            col = lax.broadcasted_iota(jnp.int32, (HD, TILE_ROWS), 1)
            run = (row == ahead * runs + col // BLOCK).astype(jnp.float32).astype(jnp.bfloat16)
            q = jnp.concatenate([q, run], axis=0)
            new_peak = jnp.full((8, TILE_ROWS), MASKED, jnp.float32)
        if kept is not None:
            total = jnp.zeros((8, TILE_ROWS), jnp.float32)
            numer = [jnp.zeros((HD, TILE_ROWS), jnp.float32) for _ in range(ACCUMULATORS)]
        for turn, at in enumerate(range(0, keys, KEY_CHUNK)):
            if ahead is not None:
                scores = jnp.dot(
                    k_all[at : at + KEY_CHUNK, :], q, preferred_element_type=jnp.float32
                )
                ahead_kept[at : at + KEY_CHUNK, :] = scores
                new_peak = jnp.maximum(new_peak, jnp.max(scores.reshape(-1, 8, TILE_ROWS), axis=0))
            if kept is not None:
                weights = jnp.exp2(kept[at : at + KEY_CHUNK, :] * scale - peak)
                total = total + jnp.sum(weights.reshape(-1, 8, TILE_ROWS), axis=0)
                numer[turn % ACCUMULATORS] += jnp.dot(
                    v_all[:, at : at + KEY_CHUNK],
                    weights.astype(jnp.bfloat16),
                    preferred_element_type=jnp.float32,
                )
        if kept is not None:
            finish(pair, odd, peak, total, functools.reduce(jnp.add, numer))
        if ahead is not None:
            return jnp.max(new_peak, axis=0, keepdims=True) * scale

    peak = advance(0, kept_a, None, None, None, None)

    def two(pair, peak):
        peak = advance(2 * pair + 1, kept_b, pair, 0, peak, kept_a)
        return advance(2 * pair + 2, kept_a, pair, 1, peak, kept_b)

    last = tiles // 2 - 1
    peak = lax.fori_loop(0, last, two, peak)
    peak = advance(tiles - 1, kept_b, last, 0, peak, kept_a)
    advance(None, None, last, 1, peak, kept_b)


def attend(q, q_rows, kv, keys_at, bias, carried, name):
    count = q.shape[0]
    chips = TILE_ROWS // q_rows
    keys = count * (keys_at[1] - keys_at[0])
    scale = math.log2(math.e) / math.sqrt(HD)
    work = count * q_rows * keys
    if carried:
        out_shape = jax.ShapeDtypeStruct((count, q_rows + q_rows // 2, HD), jnp.bfloat16)
    else:
        out_shape = jax.ShapeDtypeStruct((count // chips, HD + 8, TILE_ROWS), jnp.float32)
    vmem = pl.BlockSpec(memory_space=pltpu.VMEM)
    return pl.pallas_call(
        functools.partial(attend_kernel, q_rows, keys_at, scale, bool(carried)),
        in_specs=[vmem] * (3 + len(carried)),
        out_specs=vmem,
        out_shape=out_shape,
        scratch_shapes=[
            pltpu.VMEM((keys, 2 * HD), jnp.bfloat16),
            pltpu.VMEM((HD, keys), jnp.bfloat16),
            pltpu.VMEM((keys, TILE_ROWS), jnp.float32),
            pltpu.VMEM((keys, TILE_ROWS), jnp.float32),
        ],
        cost_estimate=pl.CostEstimate(
            flops=8 * work * HD, bytes_accessed=4 * 1024 * 1024, transcendentals=work
        ),
        compiler_params=pltpu.CompilerParams(vmem_limit_bytes=VMEM_LIMIT),
        name=name,
    )(q, kv, bias, *carried)


def project_kernel(half, which_ref, attended_ref, w_ref, out_ref, left, held, acc, sems):
    pairs = attended_ref.shape[0] // 2
    columns = out_ref.shape[1]
    pieces = sems.shape[0]
    depth = w_ref.shape[0] // pieces
    base = pl.multiple_of(which_ref[0] * columns, HD)
    copies = [
        pltpu.make_async_copy(
            w_ref.at[pl.ds(i * depth, depth), pl.ds(base, columns)],
            held.at[pl.ds(i * depth, depth), :],
            sems.at[i],
        )
        for i in range(pieces)
    ]
    for copy in copies:
        copy.start()
    for j in range(pairs):
        at = 3 * j * HD
        left[:, at : at + HD] = attended_ref[2 * j, half:, :]
        left[:half, at + HD : at + 2 * HD] = attended_ref[2 * j, :half, :]
        left[half:, at + HD : at + 2 * HD] = attended_ref[2 * j + 1, :half, :]
        left[:, at + 2 * HD : at + 3 * HD] = attended_ref[2 * j + 1, half:, :]
    for i, copy in enumerate(copies):
        copy.wait()
        rows = slice(i * depth, (i + 1) * depth)
        for n in range(0, columns, PROJECT_COLUMNS):
            here = slice(n, n + PROJECT_COLUMNS)
            part = jnp.dot(left[:, rows], held[rows, here], preferred_element_type=jnp.float32)
            if i > 0:
                part = acc[:, here] + part
            if i + 1 < pieces:
                acc[:, here] = part
            else:
                out_ref[:, here] = part.astype(out_ref.dtype)


def project(attended, half, weight, which, columns, dtype, name):
    vmem = pl.BlockSpec(memory_space=pltpu.VMEM)
    return pl.pallas_call(
        functools.partial(project_kernel, half),
        in_specs=[
            pl.BlockSpec(memory_space=pltpu.SMEM),
            vmem,
            pl.BlockSpec(memory_space=pl.ANY),
        ],
        out_specs=vmem,
        out_shape=jax.ShapeDtypeStruct((2 * half, columns), dtype),
        scratch_shapes=[
            pltpu.VMEM((2 * half, weight.shape[0]), jnp.bfloat16),
            pltpu.VMEM((weight.shape[0], columns), jnp.bfloat16),
            pltpu.VMEM((2 * half, columns), jnp.float32),
            pltpu.SemaphoreType.DMA((PROJECT_PIECES,)),
        ],
        cost_estimate=pl.CostEstimate(
            flops=4 * half * weight.shape[0] * columns,
            bytes_accessed=2 * weight.shape[0] * columns,
            transcendentals=0,
        ),
        compiler_params=pltpu.CompilerParams(vmem_limit_bytes=VMEM_LIMIT),
        name=name,
    )(which, attended, weight)


def dealt_body(
    queries,
    window_keys,
    window_values,
    context_keys,
    context_values,
    block_group,
    sees,
    out_weight,
    gate,
):
    tok_rows = queries.shape[0]
    ctx_rows = context_keys.shape[0]
    tm_count = lax.axis_size("tm")
    own_index = lax.axis_index("tm")
    core = lax.axis_index("head")
    side = own_index % 2
    half_q, half_c = tok_rows // 2, ctx_rows // 2

    arrays = [
        pltpu.with_memory_space_constraint(x, pltpu.HBM)
        for x in (queries, context_keys, window_keys, context_values, window_values)
    ]
    shared = lax.all_to_all(pack(arrays, False, "pack_shared"), "tm", 0, 0, tiled=True)
    own = lax.all_to_all(pack(arrays, True, "pack_own"), "tm", 0, 0, tiled=True)

    table = sees.astype(jnp.float32)
    groups = jnp.arange(sees.shape[0], dtype=jnp.int32)
    picks = (block_group[:, None] == groups[None, :]).astype(jnp.float32)
    ctx_blocks = ctx_rows * tm_count // BLOCK
    seen_by = picks @ table.T @ picks[ctx_blocks:].T
    bias = jnp.where(seen_by > 0.5, jnp.float32(0.0), jnp.float32(MASKED))
    n_query_blocks = bias.shape[1]
    bias = jnp.concatenate(
        [
            bias[:ctx_blocks].reshape(tm_count, -1, n_query_blocks),
            bias[ctx_blocks:].reshape(tm_count, -1, n_query_blocks),
        ],
        axis=1,
    )
    pad = lambda x: jnp.pad(x, ((0, 0), (0, HD - x.shape[1])))
    own_bias = pad(bias.reshape(-1, n_query_blocks))
    c_blocks, q_blocks = half_c // BLOCK, half_q // BLOCK
    near = jnp.where(
        side == 0,
        jnp.concatenate(
            [bias[:, :c_blocks], bias[:, 2 * c_blocks : 2 * c_blocks + q_blocks]], axis=1
        ),
        jnp.concatenate(
            [bias[:, c_blocks : 2 * c_blocks], bias[:, 2 * c_blocks + q_blocks :]], axis=1
        ),
    ).reshape(-1, tm_count, 2, q_blocks)
    flat = lambda x: pad(x.reshape(x.shape[0], -1))
    lo, hi = flat(near[:, :, 0]), flat(near[:, :, 1])
    my_bias = jnp.where(side == 0, lo, hi)
    their_bias = jnp.where(side == 0, hi, lo)

    swap = [(i, i ^ 1) for i in range(tm_count)]
    half_kv, full_kv = half_c + half_q, ctx_rows + tok_rows
    shared_at = (half_q, half_q + half_kv, half_q + half_kv, half_q + 2 * half_kv)
    own_at = (tok_rows, tok_rows + full_kv, tok_rows + full_kv, tok_rows + 2 * full_kv)
    their_q = lax.ppermute(shared[:, :half_q, :], "tm", swap)
    mine = attend(shared, half_q, shared, shared_at, my_bias, (), "attend_mine")
    theirs = attend(their_q, half_q, shared, shared_at, their_bias, (), "attend_theirs")
    theirs = lax.ppermute(theirs, "tm", swap)
    attended = attend(own, tok_rows, own, own_at, own_bias, (mine, theirs), "attend_own")
    attended = lax.all_to_all(attended, "tm", 0, 0, tiled=True)

    columns = gate.shape[0]
    other = (1 - core).astype(jnp.int32).reshape(1)
    this = core.astype(jnp.int32).reshape(1)
    weight = pltpu.with_memory_space_constraint(out_weight, pltpu.HBM)
    sent = project(attended, half_q, weight, other, columns, jnp.bfloat16, "project_theirs")
    got = lax.ppermute(sent, "head", [(0, 1), (1, 0)])
    kept = project(attended, half_q, weight, this, columns, jnp.float32, "project_mine")
    return (gate[None, :] * (kept + got.astype(jnp.float32))).astype(jnp.bfloat16)


def body(queries, window_keys, window_values, context_keys, *rest):
    tm_count = lax.axis_size("tm")
    local_heads = queries.shape[1] // HD
    halves = (queries.shape[0] // 2, context_keys.shape[0] // 2)
    dealt = (
        2 * local_heads == 3 * tm_count
        and lax.axis_size("head") == 2
        and all(h % BLOCK == 0 for h in halves)
        and TILE_ROWS % (2 * halves[0]) == 0
        and halves[0] * tm_count % TILE_ROWS == 0
        and tm_count * queries.shape[0] % (4 * TILE_ROWS) == 0
        and queries.shape[1] % PROJECT_COLUMNS == 0
        and queries.shape[1] % (PROJECT_PIECES * HD) == 0
        and queries.shape[0] * tm_count // BLOCK <= HD
    )
    chosen = dealt_body if dealt else gathered_body
    return chosen(queries, window_keys, window_values, context_keys, *rest)


def solution(mesh):
    placed = (
        P("tm", "head"),
        P("tm", "head"),
        P("tm", "head"),
        P("tm", "head"),
        P("tm", "head"),
        P(),
        P(),
        P("head", None),
        P("head"),
    )
    return jax.shard_map(
        body, mesh=mesh, in_specs=placed, out_specs=P("tm", "head"), check_vma=False
    )
```

```python
import functools
import math

import jax
import jax.numpy as jnp
from jax import lax
from jax.experimental import pallas as pl
from jax.experimental.pallas import tpu as pltpu
from jax.sharding import PartitionSpec as P

HD = 128
BLOCK = 64
MASKED = -1e30
VMEM_LIMIT = 40 * 1024 * 1024
TILE_ROWS = 4 * BLOCK
KEY_CHUNK = 256
ACCUMULATORS = 2
PROJECT_COLUMNS = 1024
PROJECT_PIECES = 6


def group_rows(positions, group_table, group_count):
    blocks = positions // BLOCK
    picker = (blocks[:, None] == jnp.arange(group_table.shape[0], dtype=jnp.int32)[None, :]).astype(
        jnp.float32
    )
    group_ids = jnp.dot(picker, group_table, precision=lax.Precision.HIGHEST)
    return (group_ids[:, None] == jnp.arange(group_count, dtype=jnp.float32)[None, :]).astype(
        jnp.float32
    )


def gathered_body(
    queries,
    window_keys,
    window_values,
    context_keys,
    context_values,
    block_group,
    sees,
    out_weight,
    gate,
):
    tok_rows = queries.shape[0]
    features = queries.shape[1]
    local_heads = features // HD
    tm_count = lax.axis_size("tm")
    own_index = lax.axis_index("tm")
    ctx_rows = context_keys.shape[0]
    ctx_total = ctx_rows * tm_count
    group_count = sees.shape[0]
    group_table = block_group.astype(jnp.float32)
    sees_table = sees.astype(jnp.float32)
    score_scale = 1.0 / jnp.sqrt(jnp.float32(HD))
    all_queries = lax.all_gather(queries, "tm", axis=0, tiled=True)
    win_rows = all_queries.shape[0]
    query_pos = ctx_total + jnp.arange(win_rows, dtype=jnp.int32)
    key_pos = jnp.concatenate(
        [
            own_index * ctx_rows + jnp.arange(ctx_rows, dtype=jnp.int32),
            ctx_total + own_index * tok_rows + jnp.arange(tok_rows, dtype=jnp.int32),
        ]
    )
    query_sees = jnp.dot(
        group_rows(query_pos, group_table, group_count), sees_table, precision=lax.Precision.HIGHEST
    )
    key_onehot = group_rows(key_pos, group_table, group_count)
    visible = jnp.dot(query_sees, key_onehot.T, precision=lax.Precision.HIGHEST) > 0.5
    key_piece = jnp.concatenate([context_keys, window_keys], axis=0).reshape(
        ctx_rows + tok_rows, local_heads, HD
    )
    value_piece = jnp.concatenate([context_values, window_values], axis=0).reshape(
        ctx_rows + tok_rows, local_heads, HD
    )
    query_heads = all_queries.reshape(win_rows, local_heads, HD)
    scores = (
        jnp.einsum("qhd,khd->hqk", query_heads, key_piece, preferred_element_type=jnp.float32)
        * score_scale
    )
    scores = jnp.where(visible[None], scores, jnp.float32(-1e30))
    row_peak = lax.pmax(jnp.max(scores, axis=-1).astype(jnp.bfloat16), "tm").astype(jnp.float32)
    weights = jnp.where(visible[None], jnp.exp(scores - row_peak[..., None]), jnp.float32(0.0))
    totals = jnp.sum(weights, axis=-1).T
    numer = jnp.einsum(
        "hqk,khd->qhd",
        weights.astype(jnp.bfloat16),
        value_piece,
        preferred_element_type=jnp.float32,
    ).reshape(win_rows, features)
    numer_mine, totals_mine = (
        lax.psum_scatter(numer.astype(jnp.bfloat16), "tm", scatter_dimension=0, tiled=True).astype(
            jnp.float32
        ),
        lax.psum_scatter(totals.astype(jnp.bfloat16), "tm", scatter_dimension=0, tiled=True).astype(
            jnp.float32
        ),
    )
    attended = (
        (numer_mine.reshape(tok_rows, local_heads, HD) / totals_mine[..., None])
        .reshape(tok_rows, features)
        .astype(jnp.bfloat16)
    )
    projected = jnp.dot(attended, out_weight, preferred_element_type=jnp.float32)
    summed = lax.psum_scatter(
        projected.astype(jnp.bfloat16), "head", scatter_dimension=1, tiled=True
    ).astype(jnp.float32)
    return (gate[None, :] * summed).astype(jnp.bfloat16)


def pack_kernel(pieces, *refs):
    n = (len(refs) - 2) // 2
    in_refs, out_ref, held, sems = refs[:n], refs[n], refs[n + 1 : -1], refs[-1]
    copies = [pltpu.make_async_copy(x, y, sems.at[i]) for i, (x, y) in enumerate(zip(in_refs, held))]
    for copy in copies:
        copy.start()
    waiting = dict(enumerate(copies))
    at = 0
    for i, whole in pieces:
        ref = held[i]
        if i in waiting:
            waiting.pop(i).wait()
        rows = ref.shape[0]
        half = rows // 2
        for j in range(ref.shape[1] // (3 * HD)):
            for side in range(2):
                if whole:
                    head = 3 * j + 2 * side
                    out_ref[2 * j + side, at : at + rows, :] = ref[:, head * HD : (head + 1) * HD]
                else:
                    head = 3 * j + 1
                    out_ref[2 * j + side, at : at + half, :] = ref[
                        side * half : (side + 1) * half, head * HD : (head + 1) * HD
                    ]
        at += rows if whole else half


def pack(arrays, pieces, name):
    groups = arrays[0].shape[1] // (3 * HD)
    total = sum(arrays[i].shape[0] // (1 if whole else 2) for i, whole in pieces)
    return pl.pallas_call(
        functools.partial(pack_kernel, pieces),
        in_specs=[pl.BlockSpec(memory_space=pl.ANY) for _ in arrays],
        out_specs=pl.BlockSpec(memory_space=pltpu.VMEM),
        out_shape=jax.ShapeDtypeStruct((2 * groups, total, HD), arrays[0].dtype),
        scratch_shapes=[pltpu.VMEM(x.shape, x.dtype) for x in arrays]
        + [pltpu.SemaphoreType.DMA((len(arrays),))],
        cost_estimate=pl.CostEstimate(
            flops=1 << 29, bytes_accessed=8 * 1024 * 1024, transcendentals=0
        ),
        compiler_params=pltpu.CompilerParams(vmem_limit_bytes=VMEM_LIMIT),
        name=name,
    )(*arrays)


def join(one, numer, total_log):
    one_log = one[HD : HD + 1, :]
    top = jnp.maximum(one_log, total_log)
    one_part, part = jnp.exp2(one_log - top), jnp.exp2(total_log - top)
    joined = (one_part * one[:HD, :] + part * numer) / (one_part + part)
    return joined.T.astype(jnp.bfloat16)


def attend_kernel(q_from, q_rows, keys_at, scale, carried, *refs):
    q_ref, kv_ref, bias_ref = refs[:3]
    if carried:
        early_ref, out_ref, k_all, v_all, kept_a, kept_b, early, sem = refs[3:]
        copy = pltpu.make_async_copy(early_ref, early, sem)
        copy.start()
    else:
        out_ref, k_all, v_all, kept_a, kept_b = refs[3:]
    keys = k_all.shape[0]
    chips = TILE_ROWS // q_rows
    runs = TILE_ROWS // BLOCK
    tiles = q_ref.shape[0] // chips

    k_lo, k_hi, v_lo, v_hi = keys_at
    count = kv_ref.shape[0]
    k_all[:, :HD] = kv_ref[:, k_lo:k_hi, :].reshape(keys, HD)
    blocks = keys // BLOCK
    k_all[:, HD:] = (
        jnp.broadcast_to(bias_ref[...][:, None, :], (blocks, BLOCK, HD))
        .reshape(keys, HD)
        .astype(jnp.bfloat16)
    )
    some = v_hi - v_lo
    for i in range(count):
        v_all[:, i * some : (i + 1) * some] = kv_ref[i, v_lo:v_hi, :].T

    def finish(pair, odd, peak, total, numer):
        total = jnp.sum(total, axis=0, keepdims=True)
        numer = numer / total
        tile = 2 * pair + odd
        total_log = peak + jnp.log2(total)
        if carried:
            skip = out_ref.shape[1] - q_rows
            joined = join(early[tile], numer, total_log)
            out_ref[pl.ds(tile * chips, chips), skip:, :] = joined.reshape(chips, q_rows, HD)
        else:
            out_ref[tile, :HD, :] = numer
            out_ref[tile, HD:, :] = jnp.broadcast_to(total_log, (8, TILE_ROWS))

    def advance(ahead, ahead_kept, pair, odd, peak, kept):
        if ahead is not None:
            q = q_ref[pl.ds(ahead * chips, chips), q_from : q_from + q_rows, :].reshape(TILE_ROWS, HD).T
            row = lax.broadcasted_iota(jnp.int32, (HD, TILE_ROWS), 0)
            col = lax.broadcasted_iota(jnp.int32, (HD, TILE_ROWS), 1)
            run = (row == ahead * runs + col // BLOCK).astype(jnp.float32).astype(jnp.bfloat16)
            q = jnp.concatenate([q, run], axis=0)
            new_peak = jnp.full((8, TILE_ROWS), MASKED, jnp.float32)
        if kept is not None:
            total = jnp.zeros((8, TILE_ROWS), jnp.float32)
            numer = [jnp.zeros((HD, TILE_ROWS), jnp.float32) for _ in range(ACCUMULATORS)]
        for turn, at in enumerate(range(0, keys, KEY_CHUNK)):
            if ahead is not None:
                scores = jnp.dot(
                    k_all[at : at + KEY_CHUNK, :], q, preferred_element_type=jnp.float32
                )
                ahead_kept[at : at + KEY_CHUNK, :] = scores
                new_peak = jnp.maximum(new_peak, jnp.max(scores.reshape(-1, 8, TILE_ROWS), axis=0))
            if kept is not None:
                weights = jnp.exp2(kept[at : at + KEY_CHUNK, :] * scale - peak)
                total = total + jnp.sum(weights.reshape(-1, 8, TILE_ROWS), axis=0)
                numer[turn % ACCUMULATORS] += jnp.dot(
                    v_all[:, at : at + KEY_CHUNK],
                    weights.astype(jnp.bfloat16),
                    preferred_element_type=jnp.float32,
                )
        if kept is not None:
            finish(pair, odd, peak, total, functools.reduce(jnp.add, numer))
        if ahead is not None:
            return jnp.max(new_peak, axis=0, keepdims=True) * scale

    peak = advance(0, kept_a, None, None, None, None)
    if carried:
        copy.wait()

    def two(pair, peak):
        peak = advance(2 * pair + 1, kept_b, pair, 0, peak, kept_a)
        return advance(2 * pair + 2, kept_a, pair, 1, peak, kept_b)

    last = tiles // 2 - 1
    peak = lax.fori_loop(0, last, two, peak)
    peak = advance(tiles - 1, kept_b, last, 0, peak, kept_a)
    advance(None, None, last, 1, peak, kept_b)


def attend(q, q_from, q_rows, kv, keys_at, bias, carried, spare, name):
    count = q.shape[0]
    chips = TILE_ROWS // q_rows
    keys = count * (keys_at[1] - keys_at[0])
    scale = math.log2(math.e) / math.sqrt(HD)
    work = count * q_rows * keys
    vmem = pl.BlockSpec(memory_space=pltpu.VMEM)
    in_specs = [vmem] * 3
    scratch = [
        pltpu.VMEM((keys, 2 * HD), jnp.bfloat16),
        pltpu.VMEM((HD, keys), jnp.bfloat16),
        pltpu.VMEM((keys, TILE_ROWS), jnp.float32),
        pltpu.VMEM((keys, TILE_ROWS), jnp.float32),
    ]
    if carried:
        in_specs += [pl.BlockSpec(memory_space=pl.ANY)]
        scratch += [pltpu.VMEM(carried[0].shape, carried[0].dtype), pltpu.SemaphoreType.DMA(())]
        carried = [pltpu.with_memory_space_constraint(x, pltpu.HBM) for x in carried]
        out_shape = pltpu.HBM((count, spare + q_rows, HD), jnp.bfloat16)
    else:
        out_shape = pltpu.HBM((count // chips, HD + 8, TILE_ROWS), jnp.float32)
    return pl.pallas_call(
        functools.partial(attend_kernel, q_from, q_rows, keys_at, scale, bool(carried)),
        in_specs=in_specs,
        out_specs=vmem,
        out_shape=out_shape,
        scratch_shapes=scratch,
        cost_estimate=pl.CostEstimate(
            flops=8 * work * HD, bytes_accessed=4 * 1024 * 1024, transcendentals=work
        ),
        compiler_params=pltpu.CompilerParams(vmem_limit_bytes=VMEM_LIMIT),
        name=name,
    )(q, kv, bias, *carried)


def join_kernel(mine_ref, theirs_ref, whole_ref, out_ref, joined, sem):
    del whole_ref
    tiles = mine_ref.shape[0]
    chips, rows = joined.shape[0] // tiles, joined.shape[1]
    for tile in range(tiles):
        theirs = theirs_ref[tile]
        joined[tile * chips : (tile + 1) * chips] = join(
            mine_ref[tile], theirs[:HD, :], theirs[HD : HD + 1, :]
        ).reshape(chips, rows, HD)
    copy = pltpu.make_async_copy(joined, out_ref.at[:, :rows, :], sem)
    copy.start()
    copy.wait()


def join_shared(mine, theirs, attended, rows):
    vmem = pl.BlockSpec(memory_space=pltpu.VMEM)
    return pl.pallas_call(
        join_kernel,
        in_specs=[vmem, vmem, pl.BlockSpec(memory_space=pl.ANY)],
        out_specs=pl.BlockSpec(memory_space=pl.ANY),
        out_shape=jax.ShapeDtypeStruct(attended.shape, attended.dtype),
        input_output_aliases={2: 0},
        scratch_shapes=[
            pltpu.VMEM((attended.shape[0], rows, HD), attended.dtype),
            pltpu.SemaphoreType.DMA(()),
        ],
        cost_estimate=pl.CostEstimate(
            flops=1 << 29, bytes_accessed=8 * mine.size, transcendentals=0
        ),
        compiler_params=pltpu.CompilerParams(vmem_limit_bytes=VMEM_LIMIT),
        name="join_shared",
    )(mine, theirs, pltpu.with_memory_space_constraint(attended, pltpu.HBM))


def project_kernel(half, which_ref, attended_ref, w_ref, out_ref, left, held, acc, sems):
    pairs = attended_ref.shape[0] // 2
    columns = out_ref.shape[1]
    pieces = sems.shape[0]
    depth = w_ref.shape[0] // pieces
    base = pl.multiple_of(which_ref[0] * columns, HD)
    copies = [
        pltpu.make_async_copy(
            w_ref.at[pl.ds(i * depth, depth), pl.ds(base, columns)],
            held.at[pl.ds(i * depth, depth), :],
            sems.at[i],
        )
        for i in range(pieces)
    ]
    for copy in copies:
        copy.start()
    for j in range(pairs):
        at = 3 * j * HD
        left[:, at : at + HD] = attended_ref[2 * j, half:, :]
        left[:half, at + HD : at + 2 * HD] = attended_ref[2 * j, :half, :]
        left[half:, at + HD : at + 2 * HD] = attended_ref[2 * j + 1, :half, :]
        left[:, at + 2 * HD : at + 3 * HD] = attended_ref[2 * j + 1, half:, :]
    for i, copy in enumerate(copies):
        copy.wait()
        rows = slice(i * depth, (i + 1) * depth)
        for n in range(0, columns, PROJECT_COLUMNS):
            here = slice(n, n + PROJECT_COLUMNS)
            part = jnp.dot(left[:, rows], held[rows, here], preferred_element_type=jnp.float32)
            if i > 0:
                part = acc[:, here] + part
            if i + 1 < pieces:
                acc[:, here] = part
            else:
                out_ref[:, here] = part.astype(out_ref.dtype)


def project(attended, half, weight, which, columns, dtype, name):
    vmem = pl.BlockSpec(memory_space=pltpu.VMEM)
    return pl.pallas_call(
        functools.partial(project_kernel, half),
        in_specs=[
            pl.BlockSpec(memory_space=pltpu.SMEM),
            vmem,
            pl.BlockSpec(memory_space=pl.ANY),
        ],
        out_specs=vmem,
        out_shape=jax.ShapeDtypeStruct((2 * half, columns), dtype),
        scratch_shapes=[
            pltpu.VMEM((2 * half, weight.shape[0]), jnp.bfloat16),
            pltpu.VMEM((weight.shape[0], columns), jnp.bfloat16),
            pltpu.VMEM((2 * half, columns), jnp.float32),
            pltpu.SemaphoreType.DMA((PROJECT_PIECES,)),
        ],
        cost_estimate=pl.CostEstimate(
            flops=4 * half * weight.shape[0] * columns,
            bytes_accessed=2 * weight.shape[0] * columns,
            transcendentals=0,
        ),
        compiler_params=pltpu.CompilerParams(vmem_limit_bytes=VMEM_LIMIT),
        name=name,
    )(which, attended, weight)


def dealt_body(
    queries,
    window_keys,
    window_values,
    context_keys,
    context_values,
    block_group,
    sees,
    out_weight,
    gate,
):
    tok_rows = queries.shape[0]
    ctx_rows = context_keys.shape[0]
    tm_count = lax.axis_size("tm")
    own_index = lax.axis_index("tm")
    core = lax.axis_index("head")
    side = own_index % 2
    half_q, half_c = tok_rows // 2, ctx_rows // 2

    arrays = [
        pltpu.with_memory_space_constraint(x, pltpu.HBM)
        for x in (queries, context_keys, window_keys, context_values, window_values)
    ]
    first = pack(arrays, [(i, False) for i in range(5)] + [(0, True), (1, True), (3, True)], "pack_first")
    first = lax.all_to_all(first, "tm", 0, 0, tiled=True)
    second = pack([arrays[2], arrays[4]], [(0, True), (1, True)], "pack_second")
    second = lax.all_to_all(second, "tm", 0, 0, tiled=True)

    table = sees.astype(jnp.float32)
    groups = jnp.arange(sees.shape[0], dtype=jnp.int32)
    picks = (block_group[:, None] == groups[None, :]).astype(jnp.float32)
    ctx_blocks = ctx_rows * tm_count // BLOCK
    seen_by = picks @ table.T @ picks[ctx_blocks:].T
    bias = jnp.where(seen_by > 0.5, jnp.float32(0.0), jnp.float32(MASKED))
    n_query_blocks = bias.shape[1]
    bias = jnp.concatenate(
        [
            bias[:ctx_blocks].reshape(tm_count, -1, n_query_blocks),
            bias[ctx_blocks:].reshape(tm_count, -1, n_query_blocks),
        ],
        axis=1,
    )
    pad = lambda x: jnp.pad(x, ((0, 0), (0, HD - x.shape[1])))
    near_end = ctx_rows // BLOCK
    ctx_bias = pad(bias[:, :near_end].reshape(-1, n_query_blocks))
    win_bias = pad(bias[:, near_end:].reshape(-1, n_query_blocks))
    c_blocks, q_blocks = half_c // BLOCK, half_q // BLOCK
    near = jnp.where(
        side == 0,
        jnp.concatenate(
            [bias[:, :c_blocks], bias[:, 2 * c_blocks : 2 * c_blocks + q_blocks]], axis=1
        ),
        jnp.concatenate(
            [bias[:, c_blocks : 2 * c_blocks], bias[:, 2 * c_blocks + q_blocks :]], axis=1
        ),
    ).reshape(-1, tm_count, 2, q_blocks)
    flat = lambda x: pad(x.reshape(x.shape[0], -1))
    lo, hi = flat(near[:, :, 0]), flat(near[:, :, 1])
    my_bias = jnp.where(side == 0, lo, hi)
    their_bias = jnp.where(side == 0, hi, lo)

    swap = [(i, i ^ 1) for i in range(tm_count)]
    half_kv = half_c + half_q
    shared_at = (half_q, half_q + half_kv, half_q + half_kv, half_q + 2 * half_kv)
    own_q = half_q + 2 * half_kv
    own_k = own_q + tok_rows
    ctx_at = (own_k, own_k + ctx_rows, own_k + ctx_rows, own_k + 2 * ctx_rows)
    win_at = (0, tok_rows, tok_rows, 2 * tok_rows)
    their_q = lax.ppermute(first[:, :half_q, :], "tm", swap)
    mine = attend(first, 0, half_q, first, shared_at, my_bias, (), 0, "attend_mine")
    theirs = attend(their_q, 0, half_q, first, shared_at, their_bias, (), 0, "attend_theirs")
    theirs = lax.ppermute(theirs, "tm", swap)
    early = attend(first, own_q, tok_rows, first, ctx_at, ctx_bias, (), 0, "attend_context")
    attended = attend(
        first, own_q, tok_rows, second, win_at, win_bias, (early,), half_q, "attend_window"
    )
    attended = join_shared(mine, theirs, attended, half_q)
    attended = lax.all_to_all(attended, "tm", 0, 0, tiled=True)

    columns = gate.shape[0]
    other = (1 - core).astype(jnp.int32).reshape(1)
    this = core.astype(jnp.int32).reshape(1)
    weight = pltpu.with_memory_space_constraint(out_weight, pltpu.HBM)
    sent = project(attended, half_q, weight, other, columns, jnp.bfloat16, "project_theirs")
    got = lax.ppermute(sent, "head", [(0, 1), (1, 0)])
    kept = project(attended, half_q, weight, this, columns, jnp.float32, "project_mine")
    return (gate[None, :] * (kept + got.astype(jnp.float32))).astype(jnp.bfloat16)


def body(queries, window_keys, window_values, context_keys, *rest):
    tm_count = lax.axis_size("tm")
    local_heads = queries.shape[1] // HD
    halves = (queries.shape[0] // 2, context_keys.shape[0] // 2)
    dealt = (
        2 * local_heads == 3 * tm_count
        and lax.axis_size("head") == 2
        and all(h % BLOCK == 0 for h in halves)
        and TILE_ROWS % (2 * halves[0]) == 0
        and halves[0] * tm_count % TILE_ROWS == 0
        and tm_count * queries.shape[0] % (4 * TILE_ROWS) == 0
        and queries.shape[1] % PROJECT_COLUMNS == 0
        and queries.shape[1] % (PROJECT_PIECES * HD) == 0
        and queries.shape[0] * tm_count // BLOCK <= HD
    )
    chosen = dealt_body if dealt else gathered_body
    return chosen(queries, window_keys, window_values, context_keys, *rest)


def solution(mesh):
    placed = (
        P("tm", "head"),
        P("tm", "head"),
        P("tm", "head"),
        P("tm", "head"),
        P("tm", "head"),
        P(),
        P(),
        P("head", None),
        P("head"),
    )
    return jax.shard_map(
        body, mesh=mesh, in_specs=placed, out_specs=P("tm", "head"), check_vma=False
    )
```

```python
import functools
import math

import jax
import jax.numpy as jnp
from jax import lax
from jax.experimental import pallas as pl
from jax.experimental.pallas import tpu as pltpu
from jax.sharding import PartitionSpec as P

HD = 128
BLOCK = 64
MASKED = -1e30
VMEM_LIMIT = 40 * 1024 * 1024
TILE_ROWS = 4 * BLOCK
KEY_CHUNK = 256
ACCUMULATORS = 2
PROJECT_COLUMNS = 1024
PROJECT_PIECES = 6


def group_rows(positions, group_table, group_count):
    blocks = positions // BLOCK
    picker = (blocks[:, None] == jnp.arange(group_table.shape[0], dtype=jnp.int32)[None, :]).astype(
        jnp.float32
    )
    group_ids = jnp.dot(picker, group_table, precision=lax.Precision.HIGHEST)
    return (group_ids[:, None] == jnp.arange(group_count, dtype=jnp.float32)[None, :]).astype(
        jnp.float32
    )


def gathered_body(
    queries,
    window_keys,
    window_values,
    context_keys,
    context_values,
    block_group,
    sees,
    out_weight,
    gate,
):
    tok_rows = queries.shape[0]
    features = queries.shape[1]
    local_heads = features // HD
    tm_count = lax.axis_size("tm")
    own_index = lax.axis_index("tm")
    ctx_rows = context_keys.shape[0]
    ctx_total = ctx_rows * tm_count
    group_count = sees.shape[0]
    group_table = block_group.astype(jnp.float32)
    sees_table = sees.astype(jnp.float32)
    score_scale = 1.0 / jnp.sqrt(jnp.float32(HD))
    all_queries = lax.all_gather(queries, "tm", axis=0, tiled=True)
    win_rows = all_queries.shape[0]
    query_pos = ctx_total + jnp.arange(win_rows, dtype=jnp.int32)
    key_pos = jnp.concatenate(
        [
            own_index * ctx_rows + jnp.arange(ctx_rows, dtype=jnp.int32),
            ctx_total + own_index * tok_rows + jnp.arange(tok_rows, dtype=jnp.int32),
        ]
    )
    query_sees = jnp.dot(
        group_rows(query_pos, group_table, group_count), sees_table, precision=lax.Precision.HIGHEST
    )
    key_onehot = group_rows(key_pos, group_table, group_count)
    visible = jnp.dot(query_sees, key_onehot.T, precision=lax.Precision.HIGHEST) > 0.5
    key_piece = jnp.concatenate([context_keys, window_keys], axis=0).reshape(
        ctx_rows + tok_rows, local_heads, HD
    )
    value_piece = jnp.concatenate([context_values, window_values], axis=0).reshape(
        ctx_rows + tok_rows, local_heads, HD
    )
    query_heads = all_queries.reshape(win_rows, local_heads, HD)
    scores = (
        jnp.einsum("qhd,khd->hqk", query_heads, key_piece, preferred_element_type=jnp.float32)
        * score_scale
    )
    scores = jnp.where(visible[None], scores, jnp.float32(-1e30))
    row_peak = lax.pmax(jnp.max(scores, axis=-1).astype(jnp.bfloat16), "tm").astype(jnp.float32)
    weights = jnp.where(visible[None], jnp.exp(scores - row_peak[..., None]), jnp.float32(0.0))
    totals = jnp.sum(weights, axis=-1).T
    numer = jnp.einsum(
        "hqk,khd->qhd",
        weights.astype(jnp.bfloat16),
        value_piece,
        preferred_element_type=jnp.float32,
    ).reshape(win_rows, features)
    numer_mine, totals_mine = (
        lax.psum_scatter(numer.astype(jnp.bfloat16), "tm", scatter_dimension=0, tiled=True).astype(
            jnp.float32
        ),
        lax.psum_scatter(totals.astype(jnp.bfloat16), "tm", scatter_dimension=0, tiled=True).astype(
            jnp.float32
        ),
    )
    attended = (
        (numer_mine.reshape(tok_rows, local_heads, HD) / totals_mine[..., None])
        .reshape(tok_rows, features)
        .astype(jnp.bfloat16)
    )
    projected = jnp.dot(attended, out_weight, preferred_element_type=jnp.float32)
    summed = lax.psum_scatter(
        projected.astype(jnp.bfloat16), "head", scatter_dimension=1, tiled=True
    ).astype(jnp.float32)
    return (gate[None, :] * summed).astype(jnp.bfloat16)


def pack_kernel(pieces, *refs):
    n = (len(refs) - 4) // 2
    in_refs, result_ref, held = refs[:n], refs[n], refs[n + 1 : 2 * n + 1]
    out_ref, sems, out_sems = refs[2 * n + 1 :]
    leaving = []
    copies = [pltpu.make_async_copy(x, y, sems.at[i]) for i, (x, y) in enumerate(zip(in_refs, held))]
    for copy in copies:
        copy.start()
    waiting = dict(enumerate(copies))
    at = 0
    for i, whole in pieces:
        ref = held[i]
        if i in waiting:
            waiting.pop(i).wait()
        rows = ref.shape[0]
        half = rows // 2
        for j in range(ref.shape[1] // (3 * HD)):
            for side in range(2):
                if whole:
                    head = 3 * j + 2 * side
                    out_ref[2 * j + side, at : at + rows, :] = ref[:, head * HD : (head + 1) * HD]
                else:
                    head = 3 * j + 1
                    out_ref[2 * j + side, at : at + half, :] = ref[
                        side * half : (side + 1) * half, head * HD : (head + 1) * HD
                    ]
        here = pl.ds(at, rows if whole else half)
        leaving.append(
            pltpu.make_async_copy(
                out_ref.at[:, here, :], result_ref.at[:, here, :], out_sems.at[len(leaving)]
            )
        )
        leaving[-1].start()
        at += rows if whole else half
    for copy in leaving:
        copy.wait()


def pack(arrays, pieces, name):
    groups = arrays[0].shape[1] // (3 * HD)
    total = sum(arrays[i].shape[0] // (1 if whole else 2) for i, whole in pieces)
    return pl.pallas_call(
        functools.partial(pack_kernel, pieces),
        in_specs=[pl.BlockSpec(memory_space=pl.ANY) for _ in arrays],
        out_specs=pl.BlockSpec(memory_space=pl.ANY),
        out_shape=pltpu.HBM((2 * groups, total, HD), arrays[0].dtype),
        scratch_shapes=[pltpu.VMEM(x.shape, x.dtype) for x in arrays]
        + [
            pltpu.VMEM((2 * groups, total, HD), arrays[0].dtype),
            pltpu.SemaphoreType.DMA((len(arrays),)),
            pltpu.SemaphoreType.DMA((len(pieces),)),
        ],
        cost_estimate=pl.CostEstimate(
            flops=1 << 29, bytes_accessed=8 * 1024 * 1024, transcendentals=0
        ),
        compiler_params=pltpu.CompilerParams(vmem_limit_bytes=VMEM_LIMIT),
        name=name,
    )(*arrays)


def join(one, numer, total_log):
    one_log = one[HD : HD + 1, :]
    top = jnp.maximum(one_log, total_log)
    one_part, part = jnp.exp2(one_log - top), jnp.exp2(total_log - top)
    joined = (one_part * one[:HD, :] + part * numer) / (one_part + part)
    return joined.T.astype(jnp.bfloat16)


def attend_kernel(q_from, q_rows, keys_at, scale, carried, *refs):
    q_ref, kv_ref, bias_ref = refs[:3]
    if carried:
        early_ref, out_ref, k_all, v_all, kept_a, kept_b, early, sem = refs[3:]
        copy = pltpu.make_async_copy(early_ref, early, sem)
        copy.start()
    else:
        out_ref, k_all, v_all, kept_a, kept_b = refs[3:]
    keys = k_all.shape[0]
    chips = TILE_ROWS // q_rows
    runs = TILE_ROWS // BLOCK
    tiles = q_ref.shape[0] // chips

    k_lo, k_hi, v_lo, v_hi = keys_at
    count = kv_ref.shape[0]
    k_all[:, :HD] = kv_ref[:, k_lo:k_hi, :].reshape(keys, HD)
    blocks = keys // BLOCK
    k_all[:, HD:] = (
        jnp.broadcast_to(bias_ref[...][:, None, :], (blocks, BLOCK, HD))
        .reshape(keys, HD)
        .astype(jnp.bfloat16)
    )
    some = v_hi - v_lo
    for i in range(count):
        v_all[:, i * some : (i + 1) * some] = kv_ref[i, v_lo:v_hi, :].T

    def finish(pair, odd, peak, total, numer):
        total = jnp.sum(total, axis=0, keepdims=True)
        numer = numer / total
        tile = 2 * pair + odd
        total_log = peak + jnp.log2(total)
        if carried:
            skip = out_ref.shape[1] - q_rows
            joined = join(early[tile], numer, total_log)
            out_ref[pl.ds(tile * chips, chips), skip:, :] = joined.reshape(chips, q_rows, HD)
        else:
            out_ref[tile, :HD, :] = numer
            out_ref[tile, HD:, :] = jnp.broadcast_to(total_log, (8, TILE_ROWS))

    def advance(ahead, ahead_kept, pair, odd, peak, kept):
        if ahead is not None:
            q = q_ref[pl.ds(ahead * chips, chips), q_from : q_from + q_rows, :].reshape(TILE_ROWS, HD).T
            row = lax.broadcasted_iota(jnp.int32, (HD, TILE_ROWS), 0)
            col = lax.broadcasted_iota(jnp.int32, (HD, TILE_ROWS), 1)
            run = (row == ahead * runs + col // BLOCK).astype(jnp.float32).astype(jnp.bfloat16)
            q = jnp.concatenate([q, run], axis=0)
            new_peak = jnp.full((8, TILE_ROWS), MASKED, jnp.float32)
        if kept is not None:
            total = jnp.zeros((8, TILE_ROWS), jnp.float32)
            numer = [jnp.zeros((HD, TILE_ROWS), jnp.float32) for _ in range(ACCUMULATORS)]
        for turn, at in enumerate(range(0, keys, KEY_CHUNK)):
            if ahead is not None:
                scores = jnp.dot(
                    k_all[at : at + KEY_CHUNK, :], q, preferred_element_type=jnp.float32
                )
                ahead_kept[at : at + KEY_CHUNK, :] = scores
                new_peak = jnp.maximum(new_peak, jnp.max(scores.reshape(-1, 8, TILE_ROWS), axis=0))
            if kept is not None:
                weights = jnp.exp2(kept[at : at + KEY_CHUNK, :] * scale - peak)
                total = total + jnp.sum(weights.reshape(-1, 8, TILE_ROWS), axis=0)
                numer[turn % ACCUMULATORS] += jnp.dot(
                    v_all[:, at : at + KEY_CHUNK],
                    weights.astype(jnp.bfloat16),
                    preferred_element_type=jnp.float32,
                )
        if kept is not None:
            finish(pair, odd, peak, total, functools.reduce(jnp.add, numer))
        if ahead is not None:
            return jnp.max(new_peak, axis=0, keepdims=True) * scale

    peak = advance(0, kept_a, None, None, None, None)
    if carried:
        copy.wait()

    def two(pair, peak):
        peak = advance(2 * pair + 1, kept_b, pair, 0, peak, kept_a)
        return advance(2 * pair + 2, kept_a, pair, 1, peak, kept_b)

    last = tiles // 2 - 1
    peak = lax.fori_loop(0, last, two, peak)
    peak = advance(tiles - 1, kept_b, last, 0, peak, kept_a)
    advance(None, None, last, 1, peak, kept_b)


def attend(q, q_from, q_rows, kv, keys_at, bias, carried, spare, name):
    count = q.shape[0]
    chips = TILE_ROWS // q_rows
    keys = count * (keys_at[1] - keys_at[0])
    scale = math.log2(math.e) / math.sqrt(HD)
    work = count * q_rows * keys
    vmem = pl.BlockSpec(memory_space=pltpu.VMEM)
    in_specs = [vmem] * 3
    scratch = [
        pltpu.VMEM((keys, 2 * HD), jnp.bfloat16),
        pltpu.VMEM((HD, keys), jnp.bfloat16),
        pltpu.VMEM((keys, TILE_ROWS), jnp.float32),
        pltpu.VMEM((keys, TILE_ROWS), jnp.float32),
    ]
    if carried:
        in_specs += [pl.BlockSpec(memory_space=pl.ANY)]
        scratch += [pltpu.VMEM(carried[0].shape, carried[0].dtype), pltpu.SemaphoreType.DMA(())]
        carried = [pltpu.with_memory_space_constraint(x, pltpu.HBM) for x in carried]
        out_shape = pltpu.HBM((count, spare + q_rows, HD), jnp.bfloat16)
    else:
        out_shape = pltpu.HBM((count // chips, HD + 8, TILE_ROWS), jnp.float32)
    return pl.pallas_call(
        functools.partial(attend_kernel, q_from, q_rows, keys_at, scale, bool(carried)),
        in_specs=in_specs,
        out_specs=vmem,
        out_shape=out_shape,
        scratch_shapes=scratch,
        cost_estimate=pl.CostEstimate(
            flops=8 * work * HD, bytes_accessed=4 * 1024 * 1024, transcendentals=work
        ),
        compiler_params=pltpu.CompilerParams(vmem_limit_bytes=VMEM_LIMIT),
        name=name,
    )(q, kv, bias, *carried)


def join_kernel(mine_ref, theirs_ref, whole_ref, out_ref, joined, sem):
    del whole_ref
    tiles = mine_ref.shape[0]
    chips, rows = joined.shape[0] // tiles, joined.shape[1]
    for tile in range(tiles):
        theirs = theirs_ref[tile]
        joined[tile * chips : (tile + 1) * chips] = join(
            mine_ref[tile], theirs[:HD, :], theirs[HD : HD + 1, :]
        ).reshape(chips, rows, HD)
    copy = pltpu.make_async_copy(joined, out_ref.at[:, :rows, :], sem)
    copy.start()
    copy.wait()


def join_shared(mine, theirs, attended, rows):
    vmem = pl.BlockSpec(memory_space=pltpu.VMEM)
    return pl.pallas_call(
        join_kernel,
        in_specs=[vmem, vmem, pl.BlockSpec(memory_space=pl.ANY)],
        out_specs=pl.BlockSpec(memory_space=pl.ANY),
        out_shape=jax.ShapeDtypeStruct(attended.shape, attended.dtype),
        input_output_aliases={2: 0},
        scratch_shapes=[
            pltpu.VMEM((attended.shape[0], rows, HD), attended.dtype),
            pltpu.SemaphoreType.DMA(()),
        ],
        cost_estimate=pl.CostEstimate(
            flops=1 << 29, bytes_accessed=8 * mine.size, transcendentals=0
        ),
        compiler_params=pltpu.CompilerParams(vmem_limit_bytes=VMEM_LIMIT),
        name="join_shared",
    )(mine, theirs, pltpu.with_memory_space_constraint(attended, pltpu.HBM))


def project_kernel(half, which_ref, attended_ref, w_ref, out_ref, left, held, acc, sems):
    pairs = attended_ref.shape[0] // 2
    columns = out_ref.shape[1]
    pieces = sems.shape[0]
    depth = w_ref.shape[0] // pieces
    base = pl.multiple_of(which_ref[0] * columns, HD)
    copies = [
        pltpu.make_async_copy(
            w_ref.at[pl.ds(i * depth, depth), pl.ds(base, columns)],
            held.at[pl.ds(i * depth, depth), :],
            sems.at[i],
        )
        for i in range(pieces)
    ]
    for copy in copies:
        copy.start()
    for j in range(pairs):
        at = 3 * j * HD
        left[:, at : at + HD] = attended_ref[2 * j, half:, :]
        left[:half, at + HD : at + 2 * HD] = attended_ref[2 * j, :half, :]
        left[half:, at + HD : at + 2 * HD] = attended_ref[2 * j + 1, :half, :]
        left[:, at + 2 * HD : at + 3 * HD] = attended_ref[2 * j + 1, half:, :]
    for i, copy in enumerate(copies):
        copy.wait()
        rows = slice(i * depth, (i + 1) * depth)
        for n in range(0, columns, PROJECT_COLUMNS):
            here = slice(n, n + PROJECT_COLUMNS)
            part = jnp.dot(left[:, rows], held[rows, here], preferred_element_type=jnp.float32)
            if i > 0:
                part = acc[:, here] + part
            if i + 1 < pieces:
                acc[:, here] = part
            else:
                out_ref[:, here] = part.astype(out_ref.dtype)


def project(attended, half, weight, which, columns, dtype, name):
    vmem = pl.BlockSpec(memory_space=pltpu.VMEM)
    return pl.pallas_call(
        functools.partial(project_kernel, half),
        in_specs=[
            pl.BlockSpec(memory_space=pltpu.SMEM),
            vmem,
            pl.BlockSpec(memory_space=pl.ANY),
        ],
        out_specs=vmem,
        out_shape=jax.ShapeDtypeStruct((2 * half, columns), dtype),
        scratch_shapes=[
            pltpu.VMEM((2 * half, weight.shape[0]), jnp.bfloat16),
            pltpu.VMEM((weight.shape[0], columns), jnp.bfloat16),
            pltpu.VMEM((2 * half, columns), jnp.float32),
            pltpu.SemaphoreType.DMA((PROJECT_PIECES,)),
        ],
        cost_estimate=pl.CostEstimate(
            flops=4 * half * weight.shape[0] * columns,
            bytes_accessed=2 * weight.shape[0] * columns,
            transcendentals=0,
        ),
        compiler_params=pltpu.CompilerParams(vmem_limit_bytes=VMEM_LIMIT),
        name=name,
    )(which, attended, weight)


def dealt_body(
    queries,
    window_keys,
    window_values,
    context_keys,
    context_values,
    block_group,
    sees,
    out_weight,
    gate,
):
    tok_rows = queries.shape[0]
    ctx_rows = context_keys.shape[0]
    tm_count = lax.axis_size("tm")
    own_index = lax.axis_index("tm")
    core = lax.axis_index("head")
    side = own_index % 2
    half_q, half_c = tok_rows // 2, ctx_rows // 2

    arrays = [
        pltpu.with_memory_space_constraint(x, pltpu.HBM)
        for x in (queries, context_keys, window_keys, context_values, window_values)
    ]
    first = pack(arrays, [(i, False) for i in range(5)] + [(0, True), (1, True), (3, True)], "pack_first")
    first = lax.all_to_all(first, "tm", 0, 0, tiled=True)
    second = pack([arrays[2], arrays[4]], [(0, True), (1, True)], "pack_second")
    second = lax.all_to_all(second, "tm", 0, 0, tiled=True)

    table = sees.astype(jnp.float32)
    groups = jnp.arange(sees.shape[0], dtype=jnp.int32)
    picks = (block_group[:, None] == groups[None, :]).astype(jnp.float32)
    ctx_blocks = ctx_rows * tm_count // BLOCK
    seen_by = picks @ table.T @ picks[ctx_blocks:].T
    bias = jnp.where(seen_by > 0.5, jnp.float32(0.0), jnp.float32(MASKED))
    n_query_blocks = bias.shape[1]
    bias = jnp.concatenate(
        [
            bias[:ctx_blocks].reshape(tm_count, -1, n_query_blocks),
            bias[ctx_blocks:].reshape(tm_count, -1, n_query_blocks),
        ],
        axis=1,
    )
    pad = lambda x: jnp.pad(x, ((0, 0), (0, HD - x.shape[1])))
    near_end = ctx_rows // BLOCK
    ctx_bias = pad(bias[:, :near_end].reshape(-1, n_query_blocks))
    win_bias = pad(bias[:, near_end:].reshape(-1, n_query_blocks))
    c_blocks, q_blocks = half_c // BLOCK, half_q // BLOCK
    near = jnp.where(
        side == 0,
        jnp.concatenate(
            [bias[:, :c_blocks], bias[:, 2 * c_blocks : 2 * c_blocks + q_blocks]], axis=1
        ),
        jnp.concatenate(
            [bias[:, c_blocks : 2 * c_blocks], bias[:, 2 * c_blocks + q_blocks :]], axis=1
        ),
    ).reshape(-1, tm_count, 2, q_blocks)
    flat = lambda x: pad(x.reshape(x.shape[0], -1))
    lo, hi = flat(near[:, :, 0]), flat(near[:, :, 1])
    my_bias = jnp.where(side == 0, lo, hi)
    their_bias = jnp.where(side == 0, hi, lo)

    swap = [(i, i ^ 1) for i in range(tm_count)]
    half_kv = half_c + half_q
    shared_at = (half_q, half_q + half_kv, half_q + half_kv, half_q + 2 * half_kv)
    own_q = half_q + 2 * half_kv
    own_k = own_q + tok_rows
    ctx_at = (own_k, own_k + ctx_rows, own_k + ctx_rows, own_k + 2 * ctx_rows)
    win_at = (0, tok_rows, tok_rows, 2 * tok_rows)
    their_q = lax.ppermute(first[:, :half_q, :], "tm", swap)
    mine = attend(first, 0, half_q, first, shared_at, my_bias, (), 0, "attend_mine")
    theirs = attend(their_q, 0, half_q, first, shared_at, their_bias, (), 0, "attend_theirs")
    theirs = lax.ppermute(theirs, "tm", swap)
    early = attend(first, own_q, tok_rows, first, ctx_at, ctx_bias, (), 0, "attend_context")
    attended = attend(
        first, own_q, tok_rows, second, win_at, win_bias, (early,), half_q, "attend_window"
    )
    attended = join_shared(mine, theirs, attended, half_q)
    attended = lax.all_to_all(attended, "tm", 0, 0, tiled=True)

    columns = gate.shape[0]
    other = (1 - core).astype(jnp.int32).reshape(1)
    this = core.astype(jnp.int32).reshape(1)
    weight = pltpu.with_memory_space_constraint(out_weight, pltpu.HBM)
    sent = project(attended, half_q, weight, other, columns, jnp.bfloat16, "project_theirs")
    got = lax.ppermute(sent, "head", [(0, 1), (1, 0)])
    kept = project(attended, half_q, weight, this, columns, jnp.float32, "project_mine")
    return (gate[None, :] * (kept + got.astype(jnp.float32))).astype(jnp.bfloat16)


def body(queries, window_keys, window_values, context_keys, *rest):
    tm_count = lax.axis_size("tm")
    local_heads = queries.shape[1] // HD
    halves = (queries.shape[0] // 2, context_keys.shape[0] // 2)
    dealt = (
        2 * local_heads == 3 * tm_count
        and lax.axis_size("head") == 2
        and all(h % BLOCK == 0 for h in halves)
        and TILE_ROWS % (2 * halves[0]) == 0
        and halves[0] * tm_count % TILE_ROWS == 0
        and tm_count * queries.shape[0] % (4 * TILE_ROWS) == 0
        and queries.shape[1] % PROJECT_COLUMNS == 0
        and queries.shape[1] % (PROJECT_PIECES * HD) == 0
        and queries.shape[0] * tm_count // BLOCK <= HD
    )
    chosen = dealt_body if dealt else gathered_body
    return chosen(queries, window_keys, window_values, context_keys, *rest)


def solution(mesh):
    placed = (
        P("tm", "head"),
        P("tm", "head"),
        P("tm", "head"),
        P("tm", "head"),
        P("tm", "head"),
        P(),
        P(),
        P("head", None),
        P("head"),
    )
    return jax.shard_map(
        body, mesh=mesh, in_specs=placed, out_specs=P("tm", "head"), check_vma=False
    )
```
